512 devices in a mesh: zero: 8 (over z), tp: 8 (over x, core), shift: 8 (over y).
Axes of the slice: x: 4, y: 8, z: 8, core: 2. Of those that a mesh axis runs over, the one named last changes fastest.
Arguments:
- train_gate: bfloat16 [16384, 8192], P(('shift', 'zero'), 'tp'), parts along dimension 0, may hold values from -0.125 to 0.125
- low_gate: bfloat16 [16384, 32], P(('shift', 'zero')), parts along dimension 0, may hold values from -0.125 to 0.125
- high_gate: bfloat16 [256, 8192], P('shift', 'tp'), parts along dimension 0, may hold values from -1 to 1
- train_up: bfloat16 [16384, 8192], P(('shift', 'zero'), 'tp'), parts along dimension 0, may hold values from -0.125 to 0.125
- low_up: bfloat16 [16384, 32], P(('shift', 'zero')), parts along dimension 0, may hold values from -0.125 to 0.125
- high_up: bfloat16 [256, 8192], P('shift', 'tp'), parts along dimension 0, may hold values from -1 to 1
- norm_train: float32 [16384], P(('shift', 'zero', 'tp')), parts along dimension 0, may hold values from 0.25 to 1.75
- norm_step: float32 [16384], P(('shift', 'zero', 'tp')), parts along dimension 0, may hold values from -0.3 to 0.3
Outputs:
- ready_gate: bfloat16 [65536, 2048], P(('shift', 'tp')), parts along dimension 0
- ready_up: bfloat16 [65536, 2048], P(('shift', 'tp')), parts along dimension 0
- serve_norm: bfloat16 [16384], P('shift'), parts along dimension 0
The draws below stay inside these ranges and needn't reach their ends.
There are 8 independent parts, one for each index of `shift`. The reference program is written for one: setup_inputs(seed, part) draws one part's arguments, and reference() takes and returns one part's arrays. A program takes and returns all parts, laid end to end along the dimension named above; each array names one. Nothing has to cross between parts.
All inputs are finite; a program needn't handle non-finite values.
Results may differ from the reference program's by a relative error of at most 0.001.
Values may be sent and summed in bfloat16 or wider, within the bound.
No kernel may reach another device: no remote copies, remote signals or barrier semaphores. Data moves between devices by JAX's collectives and lax.ppermute only.
A program may use at most 64 MiB of HBM per device.

```python
import jax
import jax.numpy as jnp

D_MODEL = 2048
D_INNER = 8192
RANK = 32


def block_levels(own_key, dims, pieces, smallest, top_value):
    loudness = 1.0
    for position, parts in pieces:
        draws = jax.random.uniform(jax.random.fold_in(jax.random.fold_in(own_key, 6), position), (parts,), jnp.float32, smallest / len(pieces), top_value / len(pieces))
        loudness = loudness * jnp.repeat(jnp.exp(draws), dims[position] // parts).reshape((-1,) + (1,) * (len(dims) - 1 - position))
    return loudness


def scatter_about(rng, extent, spread, limit, pieces=(), kind=jnp.bfloat16):
    array = jax.random.normal(rng, extent, jnp.float32) * spread
    if len(pieces) > 0:
        array = block_levels(rng, extent, pieces, -0.22, 0.18) * array
    return jnp.clip(array, min=-limit, max=limit).astype(kind)


def setup_inputs(seed: int = 0, part: int = 0) -> dict:
    arg_keys = jax.random.split(jax.random.key(seed), 9)
    part_keys = jax.random.split(jax.random.fold_in(arg_keys[8], part), 9)
    return {
        "train_gate": scatter_about(part_keys[0], (D_MODEL, D_INNER), D_MODEL ** -0.5, 0.125, ((0, 8), (1, 8))),
        "low_gate": scatter_about(part_keys[1], (D_MODEL, RANK), D_MODEL ** -0.5, 0.125, ((0, 8),)),
        "high_gate": scatter_about(part_keys[2], (RANK, D_INNER), RANK ** -0.5, 1.0, ((1, 8),)),
        "train_up": scatter_about(part_keys[3], (D_MODEL, D_INNER), D_MODEL ** -0.5, 0.125, ((0, 8), (1, 8))),
        "low_up": scatter_about(part_keys[4], (D_MODEL, RANK), D_MODEL ** -0.5, 0.125, ((0, 8),)),
        "high_up": scatter_about(part_keys[5], (RANK, D_INNER), RANK ** -0.5, 1.0, ((1, 8),)),
        "norm_train": jnp.clip(1.0 + 0.15 * jax.random.normal(part_keys[6], (D_MODEL,), jnp.float32), 0.25, 1.75),
        "norm_step": jnp.clip(jax.random.uniform(part_keys[7], (D_MODEL,), jnp.float32, -0.3, 0.3) * block_levels(part_keys[7], (D_MODEL,), ((0, 64),), -0.4, 0.0), -0.3, 0.3),
    }


mix_rate = 0.5


def reference(train_gate, low_gate, high_gate, train_up, low_up, high_up, norm_train, norm_step):
    latest_gate = train_gate.astype(jnp.float32) + mix_rate * jnp.dot(low_gate, high_gate, preferred_element_type=jnp.float32)
    latest_up = train_up.astype(jnp.float32) + mix_rate * jnp.dot(low_up, high_up, preferred_element_type=jnp.float32)
    ready_gate = latest_gate.T.astype(jnp.bfloat16)
    ready_up = latest_up.T.astype(jnp.bfloat16)
    serve_norm = (norm_train + norm_step).astype(jnp.bfloat16)
    return ready_gate, ready_up, serve_norm
```

```python
import jax
import jax.numpy as jnp
from jax import lax
from jax.experimental import pallas as pl
from jax.experimental.pallas import tpu as pltpu
from jax.sharding import PartitionSpec as P

mix_rate = 0.5


def merge_kernel(train, low_t, high, out):
    product = lax.dot_general(
        low_t[...], high[...], (((0,), (0,)), ((), ())), preferred_element_type=jnp.float32
    )
    latest = train[...].astype(jnp.float32) + mix_rate * product
    out[...] = latest.astype(jnp.bfloat16).T


def merged_transpose(train, low, high):
    rows, cols = train.shape
    rank = low.shape[1]
    block = min(cols, 256)
    return pl.pallas_call(
        merge_kernel,
        grid=(cols // block,),
        in_specs=[
            pl.BlockSpec((rows, block), lambda i: (0, i)),
            pl.BlockSpec((rank, rows), lambda i: (0, 0)),
            pl.BlockSpec((rank, block), lambda i: (0, i)),
        ],
        out_specs=pl.BlockSpec((block, rows), lambda i: (i, 0)),
        out_shape=jax.ShapeDtypeStruct((cols, rows), jnp.bfloat16),
        name="merge",
    )(train, low.T, high)


def ring_pieces(piece, axis, ups):
    count = lax.axis_size(axis)
    upward = [(i, (i + 1) % count) for i in range(count)]
    downward = [(i, (i - 1) % count) for i in range(count)]
    held = {0: piece}
    for step in range(1, ups + 1):
        held[-step] = lax.ppermute(held[1 - step], axis, upward)
        if step <= count - 1 - ups:
            held[step] = lax.ppermute(held[step - 1], axis, downward)
    for step in range(ups + 1, count - ups):
        held[step] = lax.ppermute(held[step - 1], axis, downward)
    return held


def assemble(sets, axis):
    count = lax.axis_size(axis)
    offsets = [sorted(s) for s in sets]
    rows, width = sets[0][0].shape
    flat = [s[o] for s, os in zip(sets, offsets) for o in os]
    places = [(k, o) for k, os in enumerate(offsets) for o in os]
    here = lax.axis_index(axis).reshape(1).astype(jnp.int32)

    def kernel(here, *refs):
        sources, outs, sems = refs[: len(flat)], refs[len(flat) : -1], refs[-1]
        copies = []
        for n, (k, o) in enumerate(places):
            at = lax.rem(here[0] + (o + count), count)
            target = outs[k].at[:, pl.ds(pl.multiple_of(at * width, width), width)]
            copies.append(pltpu.make_async_copy(sources[n], target, sems.at[n]))
        for c in copies:
            c.start()
        for c in copies:
            c.wait()

    shape = jax.ShapeDtypeStruct((rows, width * count), jnp.bfloat16)
    return pl.pallas_call(
        kernel,
        in_specs=[pl.BlockSpec(memory_space=pltpu.SMEM)]
        + [pl.BlockSpec(memory_space=pl.ANY)] * len(flat),
        out_specs=[pl.BlockSpec(memory_space=pl.ANY)] * len(sets),
        out_shape=[shape] * len(sets),
        scratch_shapes=[pltpu.SemaphoreType.DMA((len(flat),))],
        name="assemble",
    )(here, *flat)


def doubled(rows, axis):
    count = lax.axis_size(axis)
    have = 1
    while have < count:
        nearer = [(i, (i - have) % count) for i in range(count)]
        rows = jnp.concatenate([rows, lax.ppermute(rows, axis, nearer)], axis=0)
        have *= 2
    here = lax.axis_index(axis)
    twice = jnp.concatenate([rows, rows], axis=0)
    return lax.dynamic_slice_in_dim(twice, lax.rem(count - here, count), count, axis=0)


def body(train_gate, low_gate, high_gate, train_up, low_up, high_up, norm_train, norm_step):
    gate = merged_transpose(train_gate, low_gate, high_gate)
    up = merged_transpose(train_up, low_up, high_up)
    half = lax.axis_size("zero") // 2
    gates = ring_pieces(gate, "zero", half)
    ups = ring_pieces(up, "zero", lax.axis_size("zero") - 1 - half)
    ready_gate, ready_up = assemble((gates, ups), "zero")
    norm = (norm_train + norm_step).astype(jnp.bfloat16)
    norm = doubled(norm[None], "tp").reshape(1, -1)
    serve_norm = doubled(norm, "zero").reshape(-1)
    return (ready_gate, ready_up, serve_norm)


def solution(mesh):
    in_specs = (
        P(("shift", "zero"), "tp"),
        P(("shift", "zero"), None),
        P("shift", "tp"),
        P(("shift", "zero"), "tp"),
        P(("shift", "zero"), None),
        P("shift", "tp"),
        P(("shift", "zero", "tp")),
        P(("shift", "zero", "tp")),
    )
    out_specs = (P(("shift", "tp"), None), P(("shift", "tp"), None), P("shift"))
    return jax.shard_map(body, mesh=mesh, in_specs=in_specs, out_specs=out_specs, check_vma=False)
```

```python
import jax
import jax.numpy as jnp
from jax import lax
from jax.experimental import pallas as pl
from jax.experimental.pallas import tpu as pltpu
from jax.sharding import PartitionSpec as P


mix_rate = 0.5
extra = 16


def merge_kernel(train, low_t, high, norm_train, norm_step, out):
    cols, lanes = train.shape[1], norm_train.shape[1]
    product = lax.dot_general(
        low_t[...], high[...], (((0,), (0,)), ((), ())), preferred_element_type=jnp.float32
    )
    latest = train[...].astype(jnp.float32) + mix_rate * product
    out[:cols, :] = latest.astype(jnp.bfloat16).T
    norm = (norm_train[...] + norm_step[...]).astype(jnp.bfloat16)
    out[cols:, :] = jnp.zeros((extra, out.shape[1]), jnp.bfloat16)
    out[cols:, :lanes] = jnp.broadcast_to(norm, (extra, lanes))


def merged_transpose(train, low, high, norm_train, norm_step):
    rows, cols = train.shape
    return pl.pallas_call(
        merge_kernel,
        out_shape=jax.ShapeDtypeStruct((cols + extra, rows), jnp.bfloat16),
        name="merge",
    )(train, low.T, high, norm_train[None], norm_step[None])


def sent(value, axis, shift):
    count = lax.axis_size(axis)
    return lax.ppermute(value, axis, [(i, (i + shift) % count) for i in range(count)])


def ring_pieces(piece, axis, ups):
    count = lax.axis_size(axis)
    held = {0: piece}
    for step in range(1, count):
        if step <= ups:
            held[-step] = sent(held[1 - step], axis, 1)
        if step <= count - 1 - ups:
            held[step] = sent(held[step - 1], axis, -1)
    return held


def place(outs, pieces, axis, direct=False, cuts=4):
    count = lax.axis_size(axis)
    width = pieces[0][2].shape[1]
    rows = pieces[0][2].shape[0] - extra
    block = rows // cuts
    given = 0 if outs is None else len(outs)
    total = given or len(pieces)

    def kernel(*refs):
        sources, targets = refs[: len(pieces)], refs[len(pieces) + given :][:total]
        staging, sems, stage_sems = refs[len(pieces) + given + total :]
        copies, stages = [], []
        for n, (k, offset, _) in enumerate(pieces):
            at = lax.rem(lax.axis_index(axis) + (offset + count), count)
            columns = pl.ds(pl.multiple_of(at * width, width), width)
            for c in range(cuts):
                some, one = pl.ds(c * block, block), n * cuts + c
                source = sources[n].at[some]
                if not direct:
                    stages.append(pltpu.make_async_copy(source, staging.at[one], stage_sems.at[one]))
                    source = staging.at[one]
                target = targets[k].at[some, columns]
                copies.append(pltpu.make_async_copy(source, target, sems.at[one]))
        for s in stages:
            s.start()
        for n, c in enumerate(copies):
            if stages:
                stages[n].wait()
            c.start()
        for c in copies:
            c.wait()

    held = [p[2] for p in pieces]
    if direct:
        held = [pltpu.with_memory_space_constraint(p, pltpu.VMEM) for p in held]
    return pl.pallas_call(
        kernel,
        in_specs=[pl.BlockSpec(memory_space=pl.ANY)] * (len(pieces) + given),
        out_specs=[pl.BlockSpec(memory_space=pl.ANY)] * total,
        out_shape=[jax.ShapeDtypeStruct((rows, width * count), jnp.bfloat16)] * total,
        input_output_aliases={len(pieces) + k: k for k in range(given)},
        scratch_shapes=[
            pltpu.VMEM((1 if direct else len(pieces) * cuts, block, width), jnp.bfloat16),
            pltpu.SemaphoreType.DMA((len(pieces) * cuts,)),
            pltpu.SemaphoreType.DMA((len(pieces) * cuts,)),
        ],
        name="place",
    )(*held, *(outs or ()))


def norms_to_send(pieces, far, axis, copies):
    count = lax.axis_size(axis)
    rows = pieces[0].shape[0]
    lanes = far.shape[1]
    offsets = sorted(pieces)

    def kernel(*refs):
        far, out, all_norms = refs[-3:]
        here = lax.axis_index(axis)
        for n, o in enumerate(offsets):
            at = lax.rem(here + (o + count), count)
            all_norms[pl.ds(at, 1), :] = refs[n][...].astype(jnp.float32)[:1, :]
        at = lax.rem(here + count // 2, count)
        all_norms[pl.ds(at, 1), :] = far[...].astype(jnp.float32)
        out[...] = jnp.broadcast_to(all_norms[...].astype(jnp.bfloat16)[None], out.shape)

    tail = pl.BlockSpec((extra, lanes), lambda i: (rows // extra - 1, 0))
    return pl.pallas_call(
        kernel,
        grid=(1,),
        in_specs=[tail] * len(offsets) + [pl.BlockSpec((1, lanes), lambda i: (0, 0))],
        out_specs=pl.BlockSpec((copies, count, lanes), lambda i: (0, 0, 0)),
        out_shape=jax.ShapeDtypeStruct((copies, count, lanes), jnp.bfloat16),
        scratch_shapes=[pltpu.VMEM((count, lanes), jnp.float32)],
        name="norms",
    )(*(pieces[o] for o in offsets), far)


def body(train_gate, low_gate, high_gate, train_up, low_up, high_up, norm_train, norm_step):
    gate = merged_transpose(train_gate, low_gate, high_gate, norm_train, norm_step)
    up = merged_transpose(train_up, low_up, high_up, norm_train, norm_step)
    count = lax.axis_size("zero")
    half = count // 2
    gates = ring_pieces(gate, "zero", half)
    ups = ring_pieces(up, "zero", count - 1 - half)
    ready = place(None, [(0, 0, gate), (1, 0, up)], "zero")
    for k in range(1, half):
        pieces = [(0, -k, gates[-k]), (1, k, ups[k]), (1, -k, ups[-k]), (0, k, gates[k])]
        ready = place(ready, pieces, "zero")
    pieces = [(0, -half, gates[-half]), (1, half, ups[half])]
    ready_gate, ready_up = place(ready, pieces, "zero", direct=True)
    lanes = norm_train.shape[0]
    own = (norm_train + norm_step).astype(jnp.bfloat16)[None]
    far = sent(jnp.pad(own, ((0, 0), (0, -lanes % 128))), "zero", half)
    near = {k: ups[k] if k > 0 else gates[k] for k in range(1 - half, half)}
    norms = norms_to_send(near, far, "zero", lax.axis_size("tp"))
    norms = lax.all_to_all(norms, "tp", 0, 0, tiled=True)
    serve_norm = norms[:, :, :lanes].swapaxes(0, 1).reshape(-1)
    return (ready_gate, ready_up, serve_norm)


def solution(mesh):
    in_specs = (
        P(("shift", "zero"), "tp"),
        P(("shift", "zero"), None),
        P("shift", "tp"),
        P(("shift", "zero"), "tp"),
        P(("shift", "zero"), None),
        P("shift", "tp"),
        P(("shift", "zero", "tp")),
        P(("shift", "zero", "tp")),
    )
    out_specs = (P(("shift", "tp"), None), P(("shift", "tp"), None), P("shift"))
    return jax.shard_map(body, mesh=mesh, in_specs=in_specs, out_specs=out_specs, check_vma=False)
```

```python
import jax
import jax.numpy as jnp
from jax import lax
from jax.experimental import pallas as pl
from jax.experimental.pallas import tpu as pltpu
from jax.sharding import PartitionSpec as P


mix_rate = 0.5
extra = 8


def merged(train, low_t, high):
    product = lax.dot_general(
        low_t[...], high[...], (((0,), (0,)), ((), ())), preferred_element_type=jnp.float32
    )
    latest = train[...].astype(jnp.float32) + mix_rate * product
    return latest.astype(jnp.bfloat16).T


def first_kernel(*refs):
    own, ahead, norms = refs[:3], refs[3:6], refs[6:8]
    out, landed = refs[8], refs[9:12]
    here, here_norms, sems = refs[12:15], refs[15:17], refs[17]
    pairs = [*zip(own, here), *zip(norms, here_norms), *zip(ahead, landed)]
    copies = [pltpu.make_async_copy(s, d, sems.at[n]) for n, (s, d) in enumerate(pairs)]
    for c in copies:
        c.start()
    for c in copies[:5]:
        c.wait()
    cols, lanes = own[0].shape[1], norms[0].shape[1]
    out[:cols, :] = merged(*here)
    norm = (here_norms[0][...] + here_norms[1][...]).astype(jnp.bfloat16)
    out[cols:, :] = jnp.zeros((extra, out.shape[1]), jnp.bfloat16)
    out[cols:, :lanes] = jnp.broadcast_to(norm, (extra, lanes))
    for c in copies[5:]:
        c.wait()


def second_kernel(train, low_t, high, beside, out):
    cols = train.shape[1]
    out[:cols, :] = merged(train, low_t, high)
    out[cols:, :] = beside[cols:, :]


def in_vmem(x):
    return pltpu.VMEM(x.shape, x.dtype)


def merged_pieces(first, second, norm_train, norm_step):
    first, second = ([t, l.T, h] for t, l, h in (first, second))
    norms = [norm_train[None], norm_step[None]]
    rows, cols = first[0].shape
    piece = pltpu.VMEM((cols + extra, rows), jnp.bfloat16)
    vmem = pl.BlockSpec(memory_space=pltpu.VMEM)
    one, *landed = pl.pallas_call(
        first_kernel,
        in_specs=[pl.BlockSpec(memory_space=pl.ANY)] * 8,
        out_specs=[vmem] * 4,
        out_shape=[piece, *(in_vmem(x) for x in second)],
        scratch_shapes=[
            *(in_vmem(x) for x in (*first, *norms)),
            pltpu.SemaphoreType.DMA((8,)),
        ],
        name="merge",
    )(*first, *second, *norms)
    other = pl.pallas_call(
        second_kernel, in_specs=[vmem] * 4, out_specs=vmem, out_shape=piece, name="merge"
    )(*(pltpu.with_memory_space_constraint(x, pltpu.VMEM) for x in (*landed, one)))
    return one, other


def sent(value, axis, shift):
    count = lax.axis_size(axis)
    return lax.ppermute(value, axis, [(i, (i + shift) % count) for i in range(count)])


def ring_pieces(piece, axis, ups):
    count = lax.axis_size(axis)
    held = {0: piece}
    for step in range(1, count):
        if step <= ups:
            held[-step] = sent(held[1 - step], axis, 1)
        if step <= count - 1 - ups:
            held[step] = sent(held[step - 1], axis, -1)
    return held


def place(outs, pieces, axis, direct=False, cuts=4):
    count = lax.axis_size(axis)
    width = pieces[0][2].shape[1]
    rows = pieces[0][2].shape[0] - extra
    block = rows // cuts
    given = 0 if outs is None else len(outs)
    total = given or len(pieces)

    def kernel(*refs):
        sources, targets = refs[: len(pieces)], refs[len(pieces) + given :][:total]
        staging, sems, stage_sems = refs[len(pieces) + given + total :]
        copies, stages = [], []
        for n, (k, offset, _) in enumerate(pieces):
            at = lax.rem(lax.axis_index(axis) + (offset + count), count)
            columns = pl.ds(pl.multiple_of(at * width, width), width)
            for c in range(cuts):
                some, one = pl.ds(c * block, block), n * cuts + c
                source = sources[n].at[some]
                if not direct:
                    stages.append(pltpu.make_async_copy(source, staging.at[one], stage_sems.at[one]))
                    source = staging.at[one]
                target = targets[k].at[some, columns]
                copies.append(pltpu.make_async_copy(source, target, sems.at[one]))
        for s in stages:
            s.start()
        for n, c in enumerate(copies):
            if stages:
                stages[n].wait()
            c.start()
        for c in copies:
            c.wait()

    held = [p[2] for p in pieces]
    if direct:
        held = [pltpu.with_memory_space_constraint(p, pltpu.VMEM) for p in held]
    return pl.pallas_call(
        kernel,
        in_specs=[pl.BlockSpec(memory_space=pl.ANY)] * (len(pieces) + given),
        out_specs=[pl.BlockSpec(memory_space=pl.ANY)] * total,
        out_shape=[jax.ShapeDtypeStruct((rows, width * count), jnp.bfloat16)] * total,
        input_output_aliases={len(pieces) + k: k for k in range(given)},
        scratch_shapes=[
            pltpu.VMEM((1 if direct else len(pieces) * cuts, block, width), jnp.bfloat16),
            pltpu.SemaphoreType.DMA((len(pieces) * cuts,)),
            pltpu.SemaphoreType.DMA((len(pieces) * cuts,)),
        ],
        name="place",
    )(*held, *(outs or ()))


def norms_to_send(pieces, far, axis, copies):
    count = lax.axis_size(axis)
    rows = pieces[0].shape[0]
    lanes = far.shape[1]
    offsets = sorted(pieces)

    def kernel(*refs):
        far, out, all_norms = refs[-3:]
        here = lax.axis_index(axis)
        for n, o in enumerate(offsets):
            at = lax.rem(here + (o + count), count)
            all_norms[pl.ds(at, 1), :] = refs[n][...].astype(jnp.float32)[:1, :]
        at = lax.rem(here + count // 2, count)
        all_norms[pl.ds(at, 1), :] = far[...].astype(jnp.float32)
        out[...] = jnp.broadcast_to(all_norms[...].astype(jnp.bfloat16)[None], out.shape)

    tail = pl.BlockSpec((extra, lanes), lambda i: (rows // extra - 1, 0))
    return pl.pallas_call(
        kernel,
        grid=(1,),
        in_specs=[tail] * len(offsets) + [pl.BlockSpec((1, lanes), lambda i: (0, 0))],
        out_specs=pl.BlockSpec((copies, count, lanes), lambda i: (0, 0, 0)),
        out_shape=jax.ShapeDtypeStruct((copies, count, lanes), jnp.bfloat16),
        scratch_shapes=[pltpu.VMEM((count, lanes), jnp.float32)],
        name="norms",
    )(*(pieces[o] for o in offsets), far)


def body(train_gate, low_gate, high_gate, train_up, low_up, high_up, norm_train, norm_step):
    gate, up = merged_pieces(
        (train_gate, low_gate, high_gate), (train_up, low_up, high_up), norm_train, norm_step
    )
    count = lax.axis_size("zero")
    half = count // 2
    gates = ring_pieces(gate, "zero", half)
    ups = ring_pieces(up, "zero", count - 1 - half)
    ready = place(None, [(0, 0, gate), (1, 0, up)], "zero", direct=True)
    for k in range(1, half):
        pieces = [(0, -k, gates[-k]), (1, k, ups[k]), (1, -k, ups[-k]), (0, k, gates[k])]
        ready = place(ready, pieces, "zero")
    pieces = [(0, -half, gates[-half]), (1, half, ups[half])]
    ready_gate, ready_up = place(ready, pieces, "zero", direct=True)
    lanes = norm_train.shape[0]
    own = (norm_train + norm_step).astype(jnp.bfloat16)[None]
    far = sent(jnp.pad(own, ((0, 0), (0, -lanes % 128))), "zero", half)
    near = {k: ups[k] if k > 0 else gates[k] for k in range(1 - half, half)}
    norms = norms_to_send(near, far, "zero", lax.axis_size("tp"))
    norms = lax.all_to_all(norms, "tp", 0, 0, tiled=True)
    serve_norm = norms[:, :, :lanes].swapaxes(0, 1).reshape(-1)
    return (ready_gate, ready_up, serve_norm)


def solution(mesh):
    in_specs = (
        P(("shift", "zero"), "tp"),
        P(("shift", "zero"), None),
        P("shift", "tp"),
        P(("shift", "zero"), "tp"),
        P(("shift", "zero"), None),
        P("shift", "tp"),
        P(("shift", "zero", "tp")),
        P(("shift", "zero", "tp")),
    )
    out_specs = (P(("shift", "tp"), None), P(("shift", "tp"), None), P("shift"))
    return jax.shard_map(body, mesh=mesh, in_specs=in_specs, out_specs=out_specs, check_vma=False)
```
